32 devices in a mesh: ctx: 2 (over core), head: 4 (over y, x), doc: 4 (over z).
Axes of the slice: x: 2, y: 2, z: 4, core: 2. Of those that a mesh axis runs over, the one named last changes fastest.
Arguments:
- queries: bfloat16 [4, 256, 8192], P('doc', 'ctx', 'head'), may hold values from -360 to 360
- keys: bfloat16 [4, 8192, 1024], P('doc', 'ctx', 'head'), may hold values from -6 to 6
- values: bfloat16 [4, 8192, 1024], P('doc', 'ctx', 'head'), may hold values from -6 to 6
- pattern: int32 [4, 2, 16], P('doc'), may hold values from 0 to 63, as said below
Outputs:
- attended: bfloat16 [4, 256, 8192], P('doc', 'ctx', 'head')
- gram: float32 [8192, 8192], P(('head', 'ctx'), 'doc')
The draws below stay inside these ranges and needn't reach their ends.
Inputs may be any that keep to these rules, and one draw needn't show every extreme that they name: Each row pattern[d, b, :] lists 16 different block numbers; no context shard (blocks s * 32 to (s + 1) * 32 - 1) holds more than 12 of one row's blocks, and in every draw some row has exactly 12 of its blocks in one shard.
All inputs are finite; a program needn't handle non-finite values.
Results may differ from the reference program's by a relative error of at most 0.015.
Values may be sent and summed in bfloat16 or wider, within the bound.
A program may use at most 128 MiB of HBM per device.

```python
import jax
import jax.numpy as jnp
from jax import lax

D = 8192
QUERY_HEADS = 64
KEY_VALUE_HEADS = 8
HEAD_SIZE = 128
BLOCK_TOKENS = 128
TOPK_DEV = 8
NKB_DEV = 32
DOCUMENT_COUNT = 4
QB = 2
QLEN = 256
CACHE_BLOCKS = 64
CONTEXT_LENGTH = 8192
SELECTED_BLOCKS = 16
CAP = 12
N_CTX = 2


def draw_queries(key, part):
    base = jax.random.truncated_normal(key, -6.0, 6.0, (DOCUMENT_COUNT, QLEN, D), jnp.float32)
    return base.astype(jnp.bfloat16)


def draw_pattern(key, part):
    rows = DOCUMENT_COUNT * QB
    owners = N_CTX
    half = owners // 2
    pair_sum = 2 * TOPK_DEV
    first_key, owner_key, local_key, order_key, force_key = jax.random.split(jax.random.fold_in(key, 11), 5)
    first = jax.random.randint(first_key, (rows, half), pair_sum - CAP, CAP + 1)
    forced_row = jax.random.randint(force_key, (), 0, rows)
    forced = (jnp.arange(rows)[:, None] == forced_row) & (jnp.arange(half)[None, :] == 0)
    first = jnp.where(forced, CAP, first)
    paired = jnp.concatenate([first, pair_sum - first], axis=1)
    owner_order = jax.vmap(lambda k: jax.random.permutation(k, owners))(jax.random.split(owner_key, rows))
    counts = jnp.take_along_axis(paired, owner_order, axis=1)
    local = jax.vmap(lambda k: jax.random.permutation(k, NKB_DEV)[:CAP])(jax.random.split(local_key, rows * owners))
    local = local.reshape(rows, owners, CAP)
    slot = jnp.arange(CAP)[None, None, :]
    valid = (slot < counts[:, :, None]).reshape(rows, owners * CAP).astype(jnp.int32)
    blocks = (jnp.arange(owners)[None, :, None] * NKB_DEV + local).reshape(rows, owners * CAP)
    shuffle = jax.vmap(lambda k: jax.random.permutation(k, owners * CAP))(jax.random.split(order_key, rows))
    score = (1 - valid) * (owners * CAP) + shuffle
    order = jnp.argsort(score, axis=1)[:, :SELECTED_BLOCKS]
    return jnp.take_along_axis(blocks, order, axis=1).reshape(DOCUMENT_COUNT, QB, SELECTED_BLOCKS).astype(jnp.int32)


def level_of(key, extent, shards, smallest, largest):
    level = 1.0
    for axis_at, shards_of in shards:
        steps = jax.random.uniform(jax.random.fold_in(jax.random.fold_in(key, 6), axis_at), (shards_of,), jnp.float32, smallest / len(shards), largest / len(shards))
        level = level * jnp.repeat(jnp.exp(steps), extent[axis_at] // shards_of).reshape((-1,) + (1,) * (len(extent) - 1 - axis_at))
    return level


def noise(key, dims, scale, bound, pieces=(), dtype=jnp.bfloat16):
    drawn = jax.random.normal(key, dims, jnp.float32) * scale
    if len(pieces) > 0:
        drawn = level_of(key, dims, pieces, -0.22, 0.18) * drawn
    return jnp.clip(drawn, min=-bound, max=bound).astype(dtype)


def setup_inputs(seed: int = 0) -> dict:
    key_of = jax.random.split(jax.random.key(seed), 5)
    queries = draw_queries(jax.random.fold_in(key_of[4], 71), 0)
    keys = noise(key_of[1], (DOCUMENT_COUNT, CONTEXT_LENGTH, KEY_VALUE_HEADS * HEAD_SIZE), 1.0, 6.0, ((0, 4), (1, 2), (2, 4)))
    values = noise(key_of[2], (DOCUMENT_COUNT, CONTEXT_LENGTH, KEY_VALUE_HEADS * HEAD_SIZE), 1.0, 6.0, ((0, 4), (1, 2), (2, 4)))
    pattern = draw_pattern(jax.random.fold_in(key_of[4], 71), 0)
    return dict(queries=queries, keys=keys, values=values, pattern=pattern)


def attend_tile(query, keys, values):
    scores = jnp.einsum("qkgd,skd->kgqs", query, keys) * (HEAD_SIZE ** -0.5)
    top = jnp.max(scores, axis=-1, keepdims=True)
    weights = jnp.exp(scores - top)
    total = jnp.sum(weights, axis=-1)
    rounded = lax.optimization_barrier(weights.astype(jnp.bfloat16))
    mixed = jnp.einsum("kgqs,skd->kgqd", rounded.astype(jnp.float32), values)
    return mixed / total[..., None]


def reference(queries, keys, values, pattern):
    every_block_list = QB * DOCUMENT_COUNT
    query_block_list = queries.reshape(every_block_list, BLOCK_TOKENS, KEY_VALUE_HEADS, QUERY_HEADS // KEY_VALUE_HEADS, HEAD_SIZE).astype(jnp.float32)
    doc_index = (jnp.arange(every_block_list) // QB).astype(jnp.int32)
    chosen = pattern.reshape(every_block_list, SELECTED_BLOCKS).astype(jnp.int32)

    def one_block(items):
        query, document_number, picked_blocks = items
        document_keys = keys[document_number].reshape(CACHE_BLOCKS, BLOCK_TOKENS, KEY_VALUE_HEADS * HEAD_SIZE)
        document_values = values[document_number].reshape(CACHE_BLOCKS, BLOCK_TOKENS, KEY_VALUE_HEADS * HEAD_SIZE)
        key_row_list = document_keys[picked_blocks].reshape(SELECTED_BLOCKS * BLOCK_TOKENS, KEY_VALUE_HEADS, HEAD_SIZE).astype(jnp.float32)
        value_row_list = document_values[picked_blocks].reshape(SELECTED_BLOCKS * BLOCK_TOKENS, KEY_VALUE_HEADS, HEAD_SIZE).astype(jnp.float32)
        mixed = attend_tile(query, key_row_list, value_row_list)
        return jnp.transpose(mixed, (2, 0, 1, 3)).reshape(BLOCK_TOKENS, D).astype(jnp.bfloat16)

    attended = lax.map(one_block, (query_block_list, doc_index, chosen)).reshape(DOCUMENT_COUNT, QLEN, D)
    flat = attended.reshape(DOCUMENT_COUNT * QLEN, D)
    gram = jnp.dot(flat.T, flat, preferred_element_type=jnp.float32)
    return attended, gram
```

```python
import functools
import math

import jax
import jax.numpy as jnp
from jax import lax
from jax.experimental import pallas as pl
from jax.experimental.pallas import tpu as pltpu
from jax.sharding import PartitionSpec as P

HEAD_SIZE = 128
BLOCK_TOKENS = 128
GROUP = 8
CAP = 12
CHUNKS = 4
MESH = pl.DeviceIdType.MESH


def slot_table(pattern, row, owner, shard_blocks, count):
    entries = pattern.shape[2]
    low = owner * shard_blocks
    seen = jnp.int32(0)
    slots = [jnp.int32(0)] * count
    for j in range(entries):
        value = pattern[0, row, j] - low
        mine = jnp.logical_and(value >= 0, value < shard_blocks)
        for s in range(min(j + 1, count)):
            slots[s] = jnp.where(jnp.logical_and(mine, seen == s), value, slots[s])
        seen = seen + jnp.where(mine, 1, 0).astype(jnp.int32)
    return slots, seen


def pack_kernel(pat, k_ref, v_ref, out_ref, sem):
    c = lax.axis_index("ctx")
    give, _ = slot_table(pat, 1 - c, c, k_ref.shape[0] // BLOCK_TOKENS, CAP)
    copies = []
    for s in range(CAP):
        there = pl.ds(pl.multiple_of(give[s] * BLOCK_TOKENS, BLOCK_TOKENS), BLOCK_TOKENS)
        here = pl.ds(s * BLOCK_TOKENS, BLOCK_TOKENS)
        for n, ref in enumerate((k_ref, v_ref)):
            copies.append(pltpu.make_async_copy(ref.at[there, :], out_ref.at[n, here, :], sem.at[n, s]))
    for copy in copies:
        copy.start()
    for copy in copies:
        copy.wait()


def swap_kernel(x_ref, out_ref, send_sem, recv_sem):
    peer = 1 - lax.axis_index("ctx")
    barrier = pltpu.get_barrier_semaphore()
    pl.semaphore_signal(barrier, inc=1, device_id={"ctx": peer}, device_id_type=MESH)
    pl.semaphore_wait(barrier, 1)
    copy = pltpu.make_async_remote_copy(
        src_ref=x_ref, dst_ref=out_ref, send_sem=send_sem, recv_sem=recv_sem,
        device_id={"ctx": peer}, device_id_type=MESH)
    copy.start()
    copy.wait()


def attend_kernel(pat, q_ref, k_ref, v_ref, far_ref, att_ref, kg, vg, sem):
    c = lax.axis_index("ctx")
    tokens, width = q_ref.shape
    entries = pat.shape[2]
    own, owned = slot_table(pat, c, c, k_ref.shape[0] // BLOCK_TOKENS, CAP)

    def block(ref, at):
        return ref.at[pl.ds(pl.multiple_of(at * BLOCK_TOKENS, BLOCK_TOKENS), BLOCK_TOKENS), :]

    def pair(p, k_src, v_src):
        here = pl.ds(p * BLOCK_TOKENS, BLOCK_TOKENS)
        return (pltpu.make_async_copy(k_src, kg.at[here, :], sem.at[0, p]),
                pltpu.make_async_copy(v_src, vg.at[here, :], sem.at[1, p]))

    for p in range(entries):
        if p < CAP:
            @pl.when(p < owned)
            def _():
                for copy in pair(p, block(k_ref, own[p]), block(v_ref, own[p])):
                    copy.start()

        @pl.when(p >= owned)
        def _():
            slot = jnp.clip(p - owned, 0, CAP - 1)
            for copy in pair(p, block(far_ref.at[0], slot), block(far_ref.at[1], slot)):
                copy.start()
    for p in range(entries):
        for copy in pair(p, block(k_ref, 0), block(v_ref, 0)):
            copy.wait()

    factor = HEAD_SIZE ** (-0.5) * math.log2(math.e)

    def two_heads(t, carry):
        at = pl.multiple_of(t * 2 * HEAD_SIZE, 2 * HEAD_SIZE)
        pair = q_ref[:, pl.ds(at, 2 * HEAD_SIZE)]
        q2 = jnp.concatenate([pair[:, :HEAD_SIZE], pair[:, HEAD_SIZE:]], axis=0)
        lane = pl.ds(pl.multiple_of((t * 2 // GROUP) * HEAD_SIZE, HEAD_SIZE), HEAD_SIZE)
        scores = lax.dot_general(q2, kg[:, lane], (((1,), (1,)), ((), ())),
                                 preferred_element_type=jnp.float32)
        top = jnp.max(scores, axis=-1, keepdims=True)
        weights = jnp.exp2((scores - top) * factor)
        total = jnp.sum(weights, axis=-1, keepdims=True)
        mixed = jnp.dot(weights.astype(jnp.bfloat16), vg[:, lane], preferred_element_type=jnp.float32)
        out = (mixed / total).astype(jnp.bfloat16)
        att_ref[:, pl.ds(at, 2 * HEAD_SIZE)] = jnp.concatenate([out[:tokens], out[tokens:]], axis=1)
        return carry

    lax.fori_loop(0, width // (2 * HEAD_SIZE), two_heads, 0)


def gather_kernel(docs, att_ref, rows_ref, cols_ref, gath, own_sem,
                  z_up, z_down, z_recv, x_send, x_recv, pr_send, pr_recv, pc_send, pc_recv, lr_sem, lc_sem):
    c = lax.axis_index("ctx")
    h = lax.axis_index("head")
    d = lax.axis_index("doc")
    peer = 1 - c
    tokens, width = att_ref.shape
    x_next = h + 1 - 2 * (h % 2)
    y_next = (h + 2) % 4
    take = pltpu.make_async_copy(att_ref, gath.at[d], own_sem)
    take.start()

    barrier = pltpu.get_barrier_semaphore()

    def greet(where):
        pl.semaphore_signal(barrier, inc=1, device_id=where, device_id_type=MESH)

    greet({"ctx": peer})
    greet({"head": x_next})
    greet({"head": y_next})

    @pl.when(d > 0)
    def _():
        greet({"doc": d - 1})

    @pl.when(d < docs - 1)
    def _():
        greet({"doc": d + 1})

    ends = jnp.where(d > 0, 1, 0) + jnp.where(d < docs - 1, 1, 0)
    pl.semaphore_wait(barrier, 3 + ends)
    take.wait()

    piece = tokens // CHUNKS
    half = width // 2
    total_events = docs * CHUNKS
    rx = (h % 2 + d % 2) % 2
    ry = (h // 2 + d // 2) % 2

    def span(k):
        return pl.ds(pl.multiple_of(k * piece, piece), piece)

    def remote(src, dst, send, recv, where):
        return pltpu.make_async_remote_copy(src_ref=src, dst_ref=dst, send_sem=send, recv_sem=recv,
                                            device_id=where, device_id_type=MESH)

    def up(i, k):
        ref = gath.at[i, span(k), :]
        return remote(ref, ref, z_up.at[i, k], z_recv.at[i, k], {"doc": d + 1})

    def down(i, k):
        ref = gath.at[i, span(k), :]
        return remote(ref, ref, z_down.at[i, k], z_recv.at[i, k], {"doc": d - 1})

    def row_copy(i, k):
        cut = pl.ds(pl.multiple_of(peer * half, half), half)
        return remote(gath.at[i, span(k), cut], rows_ref.at[i, c, span(k), :],
                      pr_send.at[i, k], pr_recv.at[i, k], {"ctx": peer})

    def row_local(i, k):
        cut = pl.ds(pl.multiple_of(c * half, half), half)
        return pltpu.make_async_copy(gath.at[i, span(k), cut], rows_ref.at[i, c, span(k), :], lr_sem.at[i, k])

    def col_local(i, k):
        return pltpu.make_async_copy(gath.at[i, span(k), :], cols_ref.at[i, c, span(k), :], lc_sem.at[i, k])

    def col_copy(i, k, src):
        return remote(src.at[span(k), :], cols_ref.at[i, c, span(k), :],
                      pc_send.at[i, k], pc_recv.at[i, k], {"ctx": peer})

    def plane_copy(i, k, src, head):
        return remote(src.at[span(k), :], cols_ref.at[i, c, span(k), :],
                      x_send.at[i, k], x_recv.at[i, k], {"head": head})

    def hop_of(par):
        first = jnp.where(par == 0, rx, ry)
        second = jnp.where(par == 0, ry, rx)
        return first + second * (3 - 2 * first)

    def next_of(par, hop):
        return jnp.where((par + hop) % 2 == 0, x_next, y_next)

    def item(side, s):
        i = d - s if side == 0 else d + s
        there = (i >= 0) if side == 0 else jnp.logical_and(i < docs, s > 0)
        return i, there

    def z_part(e):
        s, k = e // CHUNKS, e % CHUNKS
        for side in range(2):
            i, there = item(side, s)

            @pl.when(jnp.logical_and(there, e < total_events))
            def _():
                @pl.when(s > 0)
                def _():
                    up(i, k).wait_recv()

                @pl.when(jnp.logical_and(i <= d, d < docs - 1))
                def _():
                    up(i, k).start()

                @pl.when(jnp.logical_and(i >= d, d > 0))
                def _():
                    down(i, k).start()

                row_copy(i, k).start()
                row_local(i, k).start()

    def x_part(e):
        par = e % 2
        hop = hop_of(par)
        ee = e - 2 * hop
        inside = jnp.logical_and(ee >= 0, ee < total_events)
        at = jnp.where(inside, ee, 0)
        s, k = at // CHUNKS, at % CHUNKS
        for side in range(2):
            i, there = item(side, s)
            there = jnp.logical_and(there, inside)

            @pl.when(jnp.logical_and(there, hop == 0))
            def _():
                plane_copy(i, k, gath.at[i], next_of(par, hop)).start()
                col_copy(i, k, gath.at[i]).start()
                col_local(i, k).start()

            @pl.when(jnp.logical_and(there, hop > 0))
            def _():
                src = cols_ref.at[i, c]
                plane_copy(i, k, src, x_next).wait_recv()

                @pl.when(hop < 3)
                def _():
                    plane_copy(i, k, src, next_of(par, hop)).start()

                col_copy(i, k, src).start()

    def event(e, carry):
        z_part(e)
        x_part(e)
        return carry

    lax.fori_loop(0, total_events + 6, event, 0)

    def finish(n, carry):
        i, k = n // CHUNKS, n % CHUNKS
        par = k % 2
        hop = hop_of(par)

        @pl.when(jnp.logical_and(i <= d, d < docs - 1))
        def _():
            up(i, k).wait_send()

        @pl.when(jnp.logical_and(i >= d, d > 0))
        def _():
            down(i, k).wait_send()

        row_copy(i, k).wait()
        row_local(i, k).wait()
        col_copy(i, k, cols_ref.at[i, c]).wait()

        @pl.when(hop < 3)
        def _():
            plane_copy(i, k, cols_ref.at[i, c], x_next).wait_send()

        @pl.when(hop == 0)
        def _():
            col_local(i, k).wait()

        return carry

    lax.fori_loop(0, total_events, finish, 0)


def attention(queries, keys, values, pattern):
    wide = keys.shape[1]
    entries = pattern.shape[2]
    bf16 = jnp.bfloat16
    vmem = pl.BlockSpec(memory_space=pltpu.VMEM)
    smem = pl.BlockSpec(memory_space=pltpu.SMEM)
    hbm = pl.BlockSpec(memory_space=pl.ANY)
    packed_shape = jax.ShapeDtypeStruct((2, CAP * BLOCK_TOKENS, wide), bf16)
    packed = pl.pallas_call(
        pack_kernel,
        out_shape=packed_shape,
        in_specs=[smem, hbm, hbm],
        out_specs=vmem,
        scratch_shapes=[pltpu.SemaphoreType.DMA((2, CAP))],
    )(pattern, keys, values)
    far = pl.pallas_call(
        swap_kernel,
        out_shape=packed_shape,
        in_specs=[hbm],
        out_specs=hbm,
        scratch_shapes=[pltpu.SemaphoreType.DMA] * 2,
        compiler_params=pltpu.CompilerParams(collective_id=0, has_side_effects=True),
    )(packed)
    return pl.pallas_call(
        attend_kernel,
        out_shape=jax.ShapeDtypeStruct(queries.shape, bf16),
        in_specs=[smem, vmem, hbm, hbm, hbm],
        out_specs=vmem,
        scratch_shapes=[pltpu.VMEM((entries * BLOCK_TOKENS, wide), bf16)] * 2
        + [pltpu.SemaphoreType.DMA((2, entries))],
    )(pattern, queries, keys, values, far)


def gathered(attended, docs):
    tokens, width = attended.shape
    bf16 = jnp.bfloat16
    vmem = pl.BlockSpec(memory_space=pltpu.VMEM)
    return pl.pallas_call(
        functools.partial(gather_kernel, docs),
        out_shape=[
            jax.ShapeDtypeStruct((docs, 2, tokens, width // 2), bf16),
            jax.ShapeDtypeStruct((docs, 2, tokens, width), bf16),
        ],
        in_specs=[pl.BlockSpec(memory_space=pl.ANY)],
        out_specs=[vmem, vmem],
        scratch_shapes=[pltpu.VMEM((docs, tokens, width), bf16), pltpu.SemaphoreType.DMA]
        + [pltpu.SemaphoreType.DMA((docs, CHUNKS))] * 11,
        compiler_params=pltpu.CompilerParams(collective_id=1, has_side_effects=True),
    )(attended)


def per_device(queries, keys, values, pattern):
    ctx_count = lax.axis_size("ctx")
    head_count = lax.axis_size("head")
    doc_count = lax.axis_size("doc")
    owner = lax.axis_index("ctx")
    tok_rows = queries.shape[1]
    width = queries.shape[2]
    direct = head_count == 4 and doc_count == 4
    attended = attention(queries[0], keys[0], values[0], pattern)
    contract = (((0,), (0,)), ((), ()))
    if direct:
        rows, cols = gathered(attended, doc_count)
        tokens = doc_count * ctx_count * tok_rows
        product = lax.dot_general(
            rows.reshape(tokens, width // ctx_count), cols.reshape(tokens, width), contract,
            preferred_element_type=jnp.float32)
        return (attended[None], product)
    sub = width // ctx_count
    model_width = width * head_count
    span = lax.all_gather(attended, "ctx", axis=0, tiled=True)
    mine_cols = lax.dynamic_slice_in_dim(span, owner * sub, sub, 1)
    full_doc = lax.all_gather(span, "head", axis=1, tiled=True)
    slice_width = model_width // doc_count
    split_cols = full_doc.reshape(tok_rows * ctx_count, doc_count, slice_width)
    column_set = lax.all_to_all(split_cols, "doc", split_axis=1, concat_axis=0, tiled=True).reshape(
        doc_count * tok_rows * ctx_count, slice_width)
    product = lax.dot_general(
        lax.all_gather(mine_cols, "doc", axis=0, tiled=True), column_set, contract,
        preferred_element_type=jnp.float32)
    return (attended[None], product)


def solution(mesh):
    placed = (
        P("doc", "ctx", "head"),
        P("doc", "ctx", "head"),
        P("doc", "ctx", "head"),
        P("doc", None, None),
    )
    return jax.shard_map(
        per_device,
        mesh=mesh,
        in_specs=placed,
        out_specs=(P("doc", "ctx", "head"), P(("head", "ctx"), "doc")),
        check_vma=False,
    )
```

```python
import functools
import math

import jax
import jax.numpy as jnp
from jax import lax
from jax.experimental import pallas as pl
from jax.experimental.pallas import tpu as pltpu
from jax.sharding import PartitionSpec as P

HEAD_SIZE = 128
BLOCK_TOKENS = 128
GROUP = 8
WIDE = 2 * HEAD_SIZE
LAG = 4
MESH = pl.DeviceIdType.MESH


def pack_kernel(pat, k_ref, v_ref, own_ref, give_ref, sem):
    c = lax.axis_index("ctx")
    entries = pat.shape[2]
    shard_blocks = k_ref.shape[0] // BLOCK_TOKENS

    def each(action, otherwise):
        for n, (row, out_ref) in enumerate(((1 - c, give_ref), (c, own_ref))):
            for p in range(entries):
                at = pat[0, row, p] - c * shard_blocks
                mine = jnp.logical_and(at >= 0, at < shard_blocks)
                here = pl.ds(p * BLOCK_TOKENS, BLOCK_TOKENS)

                @pl.when(mine)
                def _():
                    there = pl.ds(pl.multiple_of(at * BLOCK_TOKENS, BLOCK_TOKENS), BLOCK_TOKENS)
                    for m, ref in enumerate((k_ref, v_ref)):
                        action(pltpu.make_async_copy(ref.at[there, :], out_ref.at[m, here, :], sem.at[n, m, p]))

                if otherwise:
                    @pl.when(jnp.logical_not(mine))
                    def _():
                        zero = jnp.zeros((BLOCK_TOKENS, k_ref.shape[1]), out_ref.dtype)
                        out_ref[0, here, :] = zero
                        out_ref[1, here, :] = zero

    each(lambda copy: copy.start(), True)
    each(lambda copy: copy.wait(), False)


def main_kernel(docs, gather, q_any, own_any, give_any, att_ref, *refs):
    if gather:
        (rows_ref, cols_ref, q_ref, own, recv, kv, in_sem, kv_send, kv_recv, gath, colbuf,
         z_up, z_down, z_recv, x_send, x_more, x_recv, r_send, r_recv, p_send, p_recv, r_local, c_local) = refs
    else:
        q_ref, own, recv, kv, in_sem, kv_send, kv_recv = refs
    c = lax.axis_index("ctx")
    h = lax.axis_index("head")
    d = lax.axis_index("doc")
    peer = 1 - c
    tokens, width = q_ref.shape
    chunks = width // WIDE
    x_next = h + 1 - 2 * (h % 2)
    y_next = (h + 2) % 4

    take_q = pltpu.make_async_copy(q_any, q_ref, in_sem.at[0])
    take_own = pltpu.make_async_copy(own_any, own, in_sem.at[1])
    take_own.start()
    take_q.start()

    barrier = pltpu.get_barrier_semaphore()

    def greet(where):
        pl.semaphore_signal(barrier, inc=1, device_id=where, device_id_type=MESH)

    greet({"ctx": peer})
    if gather:
        greet({"head": x_next})
        greet({"head": y_next})

        @pl.when(d > 0)
        def _():
            greet({"doc": d - 1})

        @pl.when(d < docs - 1)
        def _():
            greet({"doc": d + 1})

        ends = jnp.where(d > 0, 1, 0) + jnp.where(d < docs - 1, 1, 0)
        pl.semaphore_wait(barrier, 3 + ends)
    else:
        pl.semaphore_wait(barrier, 1)

    def remote(src, dst, send, arrive, where):
        return pltpu.make_async_remote_copy(src_ref=src, dst_ref=dst, send_sem=send, recv_sem=arrive,
                                            device_id=where, device_id_type=MESH)

    swaps = [remote(give_any.at[n], recv.at[n], kv_send.at[n], kv_recv.at[n], {"ctx": peer}) for n in range(2)]
    for swap in swaps:
        swap.start()
    take_q.wait()
    take_own.wait()
    for n, swap in enumerate(swaps):
        swap.wait()
        kv[n] = own[n] + recv[n]

    factor = HEAD_SIZE ** (-0.5) * math.log2(math.e)

    def two_heads(t):
        at = pl.multiple_of(t * WIDE, WIDE)
        pair = q_ref[:, pl.ds(at, WIDE)]
        q2 = jnp.concatenate([pair[:, :HEAD_SIZE], pair[:, HEAD_SIZE:]], axis=0)
        lane = pl.ds(pl.multiple_of((t * 2 // GROUP) * HEAD_SIZE, HEAD_SIZE), HEAD_SIZE)
        scores = lax.dot_general(q2, kv[0, :, lane], (((1,), (1,)), ((), ())),
                                 preferred_element_type=jnp.float32)
        top = jnp.max(scores, axis=-1, keepdims=True)
        weights = jnp.exp2((scores - top) * factor)
        total = jnp.sum(weights, axis=-1, keepdims=True)
        mixed = jnp.dot(weights.astype(jnp.bfloat16), kv[1, :, lane], preferred_element_type=jnp.float32)
        out = (mixed / total).astype(jnp.bfloat16)
        out = jnp.concatenate([out[:tokens], out[tokens:]], axis=1)
        if gather:
            gath[d, t] = out
        att_ref[:, pl.ds(at, WIDE)] = out

    if not gather:
        def plain(t, carry):
            two_heads(t)
            return carry

        lax.fori_loop(0, chunks, plain, 0)
        return

    total_events = docs * chunks
    far_step = docs // 2
    half_chunks = chunks // 2
    rx = (h % 2 + d % 2) % 2
    ry = (h // 2 + d // 2) % 2

    def columns(k):
        return pl.ds(pl.multiple_of(k * WIDE, WIDE), WIDE)

    def up(i, k):
        return remote(gath.at[i, k], gath.at[i, k], z_up.at[i, k], z_recv.at[i, k], {"doc": d + 1})

    def down(i, k):
        return remote(gath.at[i, k], gath.at[i, k], z_down.at[i, k], z_recv.at[i, k], {"doc": d - 1})

    def row_home(i, k):
        return rows_ref.at[i, c, :, columns(k % half_chunks)]

    def row_copy(i, k):
        return remote(gath.at[i, k], row_home(i, k), r_send.at[i, k], r_recv.at[i, k], {"ctx": peer})

    def row_local(i, k):
        return pltpu.make_async_copy(gath.at[i, k], row_home(i, k), r_local.at[i, k])

    def col_local(i, k, src):
        return pltpu.make_async_copy(src.at[i, k], cols_ref.at[i, c, :, columns(k)], c_local.at[i, k])

    def col_copy(i, k, src):
        return remote(src.at[i, k], cols_ref.at[i, c, :, columns(k)],
                      p_send.at[i, k], p_recv.at[i, k], {"ctx": peer})

    def plane_copy(i, k, src, sem, head):
        return remote(src.at[i, k], colbuf.at[i, k], sem.at[i, k], x_recv.at[i, k], {"head": head})

    def place(k):
        even = k % 2 == 0
        return (jnp.where(even, rx, ry), jnp.where(even, ry, rx),
                jnp.where(even, x_next, y_next), jnp.where(even, y_next, x_next))

    def item(side, s):
        i = d - s if side == 0 else d + s
        there = (i >= 0) if side == 0 else jnp.logical_and(i < docs, s > 0)
        return i, there

    def z_part(e):
        s, k = e // chunks, e % chunks
        for side in range(2):
            i, there = item(side, s)

            @pl.when(jnp.logical_and(there, e < total_events))
            def _():
                @pl.when(s > 0)
                def _():
                    up(i, k).wait_recv()

                @pl.when(jnp.logical_and(i <= d, d < docs - 1))
                def _():
                    up(i, k).start()

                @pl.when(jnp.logical_and(i >= d, d > 0))
                def _():
                    down(i, k).start()

                @pl.when(k // half_chunks == c)
                def _():
                    row_local(i, k).start()

                @pl.when(k // half_chunks != c)
                def _():
                    row_copy(i, k).start()

    def x_part(e):
        a, b, first, second = place(e)
        hop = a + b * (3 - 2 * a)
        ee = e - LAG * hop
        inside = jnp.logical_and(ee >= 0, ee < total_events)
        at = jnp.where(inside, ee, 0)
        s, k = at // chunks, at % chunks
        near = s < far_step
        for side in range(2):
            i, there = item(side, s)
            there = jnp.logical_and(there, inside)

            @pl.when(jnp.logical_and(there, hop == 0))
            def _():
                plane_copy(i, k, gath, x_send, first).start()

                @pl.when(s >= far_step)
                def _():
                    plane_copy(i, k, gath, x_more, second).start()

                col_copy(i, k, gath).start()
                col_local(i, k, gath).start()

            @pl.when(jnp.logical_and(there, hop > 0))
            def _():
                plane_copy(i, k, colbuf, x_send, first).wait_recv()

                @pl.when(hop == 1)
                def _():
                    plane_copy(i, k, colbuf, x_send, second).start()

                @pl.when(jnp.logical_and(hop == 2, near))
                def _():
                    plane_copy(i, k, colbuf, x_send, first).start()

                col_copy(i, k, colbuf).start()
                col_local(i, k, colbuf).start()

    def opening(e, carry):
        two_heads(e)
        z_part(e)
        x_part(e)
        return carry

    def event(e, carry):
        z_part(e)
        x_part(e)
        return carry

    lax.fori_loop(0, chunks, opening, 0)
    lax.fori_loop(chunks, total_events + 3 * LAG, event, 0)

    def finish(n, carry):
        i, k = n // chunks, n % chunks
        a, b, first, second = place(k)
        hop = a + b * (3 - 2 * a)
        near = jnp.logical_and(i - d < far_step, d - i < far_step)

        @pl.when(jnp.logical_and(i <= d, d < docs - 1))
        def _():
            up(i, k).wait_send()

        @pl.when(jnp.logical_and(i >= d, d > 0))
        def _():
            down(i, k).wait_send()

        @pl.when(k // half_chunks == c)
        def _():
            row_local(i, k).wait()
            row_copy(i, k).wait_recv()

        @pl.when(k // half_chunks != c)
        def _():
            row_copy(i, k).wait_send()

        col_copy(i, k, colbuf).wait()
        col_local(i, k, colbuf).wait()

        @pl.when(jnp.logical_or(hop < 2, jnp.logical_and(hop == 2, near)))
        def _():
            plane_copy(i, k, colbuf, x_send, first).wait_send()

        @pl.when(jnp.logical_and(hop == 0, jnp.logical_not(near)))
        def _():
            plane_copy(i, k, colbuf, x_more, second).wait_send()

        return carry

    lax.fori_loop(0, total_events, finish, 0)


def fused(queries, keys, values, pattern, docs, gather):
    tokens, width = queries.shape
    wide = keys.shape[1]
    entries = pattern.shape[2]
    bf16 = jnp.bfloat16
    vmem = pl.BlockSpec(memory_space=pltpu.VMEM)
    smem = pl.BlockSpec(memory_space=pltpu.SMEM)
    hbm = pl.BlockSpec(memory_space=pl.ANY)
    pack = (2, entries * BLOCK_TOKENS, wide)
    own, give = pl.pallas_call(
        pack_kernel,
        out_shape=[jax.ShapeDtypeStruct(pack, bf16)] * 2,
        in_specs=[smem, hbm, hbm],
        out_specs=[vmem] * 2,
        scratch_shapes=[pltpu.SemaphoreType.DMA((2, 2, entries))],
    )(pattern, keys, values)
    out_shape = [jax.ShapeDtypeStruct((tokens, width), bf16)]
    scratch = [pltpu.VMEM((tokens, width), bf16)] + [pltpu.VMEM(pack, bf16)] * 3
    scratch += [pltpu.SemaphoreType.DMA((2,))] * 3
    if gather:
        chunks = width // WIDE
        out_shape += [
            jax.ShapeDtypeStruct((docs, 2, tokens, width // 2), bf16),
            jax.ShapeDtypeStruct((docs, 2, tokens, width), bf16),
        ]
        scratch += [pltpu.VMEM((docs, chunks, tokens, WIDE), bf16)] * 2
        scratch += [pltpu.SemaphoreType.DMA((docs, chunks))] * 12
    return pl.pallas_call(
        functools.partial(main_kernel, docs, gather),
        out_shape=out_shape,
        in_specs=[hbm] * 3,
        out_specs=[vmem] + [hbm] * (len(out_shape) - 1),
        scratch_shapes=scratch,
        compiler_params=pltpu.CompilerParams(collective_id=0, has_side_effects=True),
    )(queries, own, give)


def per_device(queries, keys, values, pattern):
    ctx_count = lax.axis_size("ctx")
    head_count = lax.axis_size("head")
    doc_count = lax.axis_size("doc")
    owner = lax.axis_index("ctx")
    tok_rows = queries.shape[1]
    width = queries.shape[2]
    direct = head_count == 4 and doc_count == 4
    made = fused(queries[0], keys[0], values[0], pattern, doc_count, direct)
    contract = (((0,), (0,)), ((), ()))
    if direct:
        attended, rows, cols = made
        tokens = doc_count * ctx_count * tok_rows
        product = lax.dot_general(
            rows.reshape(tokens, width // ctx_count), cols.reshape(tokens, width), contract,
            preferred_element_type=jnp.float32)
        return (attended[None], product)
    attended = made[0]
    sub = width // ctx_count
    model_width = width * head_count
    span = lax.all_gather(attended, "ctx", axis=0, tiled=True)
    mine_cols = lax.dynamic_slice_in_dim(span, owner * sub, sub, 1)
    full_doc = lax.all_gather(span, "head", axis=1, tiled=True)
    slice_width = model_width // doc_count
    split_cols = full_doc.reshape(tok_rows * ctx_count, doc_count, slice_width)
    column_set = lax.all_to_all(split_cols, "doc", split_axis=1, concat_axis=0, tiled=True).reshape(
        doc_count * tok_rows * ctx_count, slice_width)
    product = lax.dot_general(
        lax.all_gather(mine_cols, "doc", axis=0, tiled=True), column_set, contract,
        preferred_element_type=jnp.float32)
    return (attended[None], product)


def solution(mesh):
    placed = (
        P("doc", "ctx", "head"),
        P("doc", "ctx", "head"),
        P("doc", "ctx", "head"),
        P("doc", None, None),
    )
    return jax.shard_map(
        per_device,
        mesh=mesh,
        in_specs=placed,
        out_specs=(P("doc", "ctx", "head"), P(("head", "ctx"), "doc")),
        check_vma=False,
    )
```
